32 devices in a mesh: cond: 2 (over x), gx: 4 (over y, core), yz: 4 (over z).
Axes of the slice: x: 2, y: 2, z: 4, core: 2. Of those that a mesh axis runs over, the one named last changes fastest.
Arguments:
- adjoint: float32 [2, 5, 32, 64, 256], P('cond', None, 'gx', 'yz'), may hold values from -6 to 6
- objective_gradient: float32 [2, 5, 32, 64, 256], P('cond', None, 'gx', 'yz'), may hold values from -6 to 6
- diagonal: float32 [32, 64, 256], P('gx', 'yz'), may hold values from 4 to 12
- flux_blocks: float32 [2, 6, 5, 5], P('cond'), may hold values from -1 to 1
- flux_sensitivity: bfloat16 [2, 5, 32, 64, 256], P('cond', None, 'gx', 'yz'), may hold values from -6 to 6
- surface_mask: int32 [32, 64, 256], P('gx', 'yz'), may hold values 0 or 1
- patch_band_slot: int32 [32, 64], P('gx', 'yz'), may hold values from 0 to 62
- design_basis: float32 [256, 128], replicated, may hold values from -0.046875 to 0.046875
- condition_weights: int32 [2], replicated, may hold values from 1 to 999, as said below
Outputs:
- smoothed: float32 [2, 5, 32, 64, 256], P('cond', None, 'gx', 'yz')
- residual: float32 [2, 5, 32, 64, 256], P('cond', None, 'gx', 'yz')
- design_gradient: float32 [4096], P(('gx', 'yz'))
The draws below stay inside these ranges and needn't reach their ends.
Inputs may be any that keep to these rules, and one draw needn't show every extreme that they name: `condition_weights`: positive integer weights; one condition has weight 999.
All inputs are finite; a program needn't handle non-finite values. No bound on the sum of `surface_mask` on one device may be relied on, other than what follows from the above.
Results may differ from the reference program's by a relative error of at most 0.0003.
Values sent between devices are 32-bit elements; how exact they have to be, the bound alone decides.
A program may use at most 64 MiB of HBM per device.

```python
import math
import jax
import jax.numpy as jnp
import numpy as np
from jax import lax

NZ = 256
NVAR = 5
BAND = 128
BAND_SLOTS = 63
COND = 2
CELLS_FIRST = 32
CELLS_SECOND = 64


def draw_condition_weights(key, part):
    drawn = jax.random.randint(jax.random.fold_in(key, 7), (COND,), 1, 1000, dtype=jnp.int32)
    chosen = jax.random.randint(jax.random.fold_in(key, 8), (), 0, COND, dtype=jnp.int32)
    return jnp.where(jnp.arange(COND, dtype=jnp.int32) == chosen, jnp.int32(999), drawn)


def touch_ends(array, own_key, least, top_value):
    longest = array.shape.index(max(array.shape))
    spots = []
    for shift in (0, 1):
        where = [jax.random.randint(jax.random.fold_in(own_key, axis), (), 0, length) for axis, length in enumerate(array.shape)]
        where[longest] = (where[longest] + shift) % array.shape[longest]
        spots.append(tuple(where))
    return array.at[spots[0]].set(least).at[spots[1]].set(top_value)


def level_of(stream_key, dims, cuts, low, high):
    level = 1.0
    for dim, blocks in cuts:
        steps = jax.random.uniform(jax.random.fold_in(jax.random.fold_in(stream_key, 6), dim), (blocks,), jnp.float32, low / len(cuts), high / len(cuts))
        level = level * jnp.repeat(jnp.exp(steps), dims[dim] // blocks).reshape((-1,) + (1,) * (len(dims) - 1 - dim))
    return level


def rank_table(count, skew):
    loads = [(1 << 20) // math.isqrt(grade ** skew) + 1 for grade in range(1, count + 1)]
    scale = 1 + sum(loads) // (1 << 30)
    return np.cumsum(np.array([max(1, weight // scale) for weight in loads]))


def ranked(own_key, extent, amount, lean):
    grid = rank_table(amount, lean)
    lot = jax.random.randint(jax.random.fold_in(own_key, 1), extent, 0, int(grid[amount - 1]))
    grade = jnp.searchsorted(jnp.asarray(grid, jnp.int32), lot, side="right")
    return jax.random.permutation(jax.random.fold_in(own_key, 2), amount)[grade].astype(jnp.int32)


def centred(key, shape, width, limit, pieces=(), kind=jnp.bfloat16):
    values = width * jax.random.normal(key, shape, jnp.float32)
    if pieces:
        values = values * level_of(key, shape, pieces, -0.22, 0.18)
    return jnp.clip(values, -limit, limit).astype(kind)


def setup_inputs(seed: int = 0) -> dict:
    streams_of = jax.random.split(jax.random.key(seed), 10)
    return {
        "adjoint": centred(streams_of[0], (COND, NVAR, CELLS_FIRST, CELLS_SECOND, NZ), 1.0, 6.0, ((0, 2), (2, 4), (3, 4)), jnp.float32),
        "objective_gradient": centred(streams_of[1], (COND, NVAR, CELLS_FIRST, CELLS_SECOND, NZ), 1.0, 6.0, ((0, 2), (2, 4), (3, 4)), jnp.float32),
        "diagonal": jnp.clip(jnp.exp(math.log(12.0) - 1.0986123 * jax.random.uniform(streams_of[2], (CELLS_FIRST, CELLS_SECOND, NZ), jnp.float32) ** level_of(streams_of[2], (CELLS_FIRST, CELLS_SECOND, NZ), ((0, 4), (1, 4)), -0.2, 0.2)), 4.0, 12.0),
        "flux_blocks": centred(streams_of[3], (COND, 6, NVAR, NVAR), (6 * NVAR) ** -0.5, 1.0, ((0, 2),), jnp.float32),
        "flux_sensitivity": centred(streams_of[4], (COND, NVAR, CELLS_FIRST, CELLS_SECOND, NZ), 1.0, 6.0, ((0, 2), (2, 4), (3, 4))),
        "surface_mask": touch_ends((jax.random.randint(streams_of[5], (CELLS_FIRST, CELLS_SECOND, NZ), 0, 4) < 1).astype(jnp.int32), jax.random.fold_in(streams_of[5], 1), 0, 1),
        "patch_band_slot": touch_ends(ranked(streams_of[6], (CELLS_FIRST, CELLS_SECOND), BAND_SLOTS, 2), jax.random.fold_in(streams_of[6], 3), 0, BAND_SLOTS - 1).astype(jnp.int32),
        "design_basis": centred(streams_of[7], (NZ, BAND), (NZ * CELLS_FIRST * CELLS_SECOND // 32) ** -0.5, 0.046875, (), jnp.float32),
        "condition_weights": draw_condition_weights(jax.random.fold_in(streams_of[9], 71), 0),
    }


relaxation = 0.8
neighbour_starts = ((2, 1, 1), (0, 1, 1), (1, 2, 1), (1, 0, 1), (1, 1, 2), (1, 1, 0))


def apply_operator(padded_field, diagonal, blocks):
    size_x = padded_field.shape[1] - 2
    size_y = padded_field.shape[2] - 2
    size_z = padded_field.shape[3] - 2
    result = diagonal * padded_field[:, 1:-1, 1:-1, 1:-1]
    for direction in range(6):
        start_x, start_y, start_z = neighbour_starts[direction]
        shifted = padded_field[:, start_x:start_x + size_x, start_y:start_y + size_y, start_z:start_z + size_z]
        result = result - jnp.einsum("ec,exyz->cxyz", blocks[direction], shifted, precision=lax.Precision.HIGHEST)
    return result


def spread_bands(slot_lookup):
    halfway = slot_lookup.shape[1] // 2
    first_half = jnp.pad(slot_lookup[:, :halfway], ((0, 1), (0, 0)))
    second_half = jnp.pad(slot_lookup[:, halfway:], ((1, 0), (0, 0)))
    return (first_half + second_half).reshape(-1)


def reference(adjoint, objective_gradient, diagonal, flux_blocks, flux_sensitivity, surface_mask, patch_band_slot, design_basis, condition_weights):
    def condition_solve(inputs):
        start_field, source, blocks, sensitivity = inputs

        def operate(values):
            return apply_operator(jnp.pad(values, ((0, 0), (1, 1), (1, 1), (1, 1))), diagonal, blocks)

        relaxed = start_field + (relaxation * (source - operate(start_field))) / diagonal
        smoothed = relaxed + (relaxation * (source - operate(relaxed))) / diagonal
        residual = source - operate(smoothed)
        surface = surface_mask.astype(jnp.float32) * jnp.sum(smoothed * sensitivity.astype(jnp.float32), axis=0)
        projected_gradient = jnp.dot(surface.reshape(-1, NZ), design_basis, precision=lax.Precision.HIGHEST, preferred_element_type=jnp.float32)
        slot_lookup = jax.ops.segment_sum(projected_gradient, patch_band_slot.reshape(-1), num_segments=BAND_SLOTS)
        return smoothed, residual, spread_bands(slot_lookup)

    smoothed, residual, gradients = lax.map(condition_solve, (adjoint, objective_gradient, flux_blocks, flux_sensitivity))
    weights_float = condition_weights.astype(jnp.float32)
    shares = weights_float / jnp.sum(weights_float)
    design_gradient = jnp.sum(shares[:, None] * gradients, axis=0)
    return smoothed, residual, design_gradient
```

```python
import functools

import jax
import jax.numpy as jnp
from jax import lax
from jax.experimental import pallas as pl
from jax.experimental.pallas import tpu as pltpu
from jax.sharding import PartitionSpec as P

NDES = 4096
RELAX = 0.8
LANES = 128
PAD = 8
MESH = pl.DeviceIdType.MESH


def kernel(
    sizes,
    adjoint,
    source_hbm,
    diagonal_hbm,
    flux,
    sensitivity_hbm,
    mask_hbm,
    slots_hbm,
    basis_hbm,
    weights,
    smoothed_out,
    residual_out,
    gradient_out,
    fields,
    source,
    diagonal,
    sensitivity,
    mask,
    slots,
    basis,
    surface,
    pieces,
    arrived,
    local_sems,
    send_sems,
    recv_sems,
    piece_sems,
):
    n_cond, n_gx, n_yz = sizes
    devices = n_cond * n_gx * n_yz
    nvar, nx, ny, nz = source.shape
    halves = nz // LANES
    rows = pieces.shape[1]
    per_owner = NDES // (n_gx * n_yz)
    ci, xi, yi = lax.axis_index("cond"), lax.axis_index("gx"), lax.axis_index("yz")
    me = (ci * n_gx + xi) * n_yz + yi

    def place(flat):
        return (flat // (n_gx * n_yz), (flat // n_yz) % n_gx, flat % n_yz)

    barrier = pltpu.get_barrier_semaphore()

    def greet(step, carry):
        pl.semaphore_signal(
            barrier, inc=1, device_id=place((me + step) % devices), device_id_type=MESH
        )
        return carry

    lax.fori_loop(1, devices, greet, 0)

    loads = []

    def load(src, dst):
        copy = pltpu.make_async_copy(src, dst, local_sems.at[len(loads)])
        copy.start()
        loads.append(copy)

    for h in range(halves):
        load(
            adjoint.at[0, :, :, :, pl.ds(h * LANES, LANES)],
            fields.at[0, :, pl.ds(1, nx), h, pl.ds(PAD, ny), :],
        )
    load(source_hbm.at[0], source)
    load(diagonal_hbm, diagonal)
    first_loads = len(loads)
    load(sensitivity_hbm.at[0], sensitivity)
    load(mask_hbm, mask)
    load(slots_hbm, slots)
    load(basis_hbm, basis)

    @pl.when(xi == 0)
    def _():
        fields[:, :, 0] = jnp.zeros_like(fields[:, :, 0])

    @pl.when(xi == n_gx - 1)
    def _():
        fields[:, :, nx + 1] = jnp.zeros_like(fields[:, :, nx + 1])

    blank = jnp.zeros((3, nvar, nx, halves, 1, LANES), jnp.float32)

    @pl.when(yi == 0)
    def _():
        fields[:, :, 1 : nx + 1, :, PAD - 1 : PAD, :] = blank

    @pl.when(yi == n_yz - 1)
    def _():
        fields[:, :, 1 : nx + 1, :, PAD + ny : PAD + ny + 1, :] = blank

    def faces(stage):
        whole_x = pl.ds(1, nx)
        plans = []
        for h in range(halves):
            lanes = pl.ds(h * LANES, LANES)

            def at(x, y, stage=stage, h=h):
                return fields.at[stage, :, x, h, y, :]

            def sent(x, y, stage=stage, lanes=lanes, h=h):
                if stage == 0:
                    x0 = x - 1 if isinstance(x, int) else pl.ds(0, nx)
                    return adjoint.at[0, :, x0, pl.ds(y.start - PAD, y.size), lanes]
                return fields.at[stage, :, x, h, y, :]

            inner_y = pl.ds(PAD, ny)
            plans.append((xi < n_gx - 1, xi > 0, (ci, xi + 1, yi), sent(nx, inner_y), at(0, inner_y)))
            plans.append((xi > 0, xi < n_gx - 1, (ci, xi - 1, yi), sent(1, inner_y), at(nx + 1, inner_y)))
            plans.append((yi < n_yz - 1, yi > 0, (ci, xi, yi + 1), sent(whole_x, pl.ds(PAD + ny - 1, 1)), at(whole_x, pl.ds(PAD - 1, 1))))
            plans.append((yi > 0, yi < n_yz - 1, (ci, xi, yi - 1), sent(whole_x, pl.ds(PAD, 1)), at(whole_x, pl.ds(PAD + ny, 1))))
        out = []
        for i, (go, come, target, src, dst) in enumerate(plans):
            copy = pltpu.make_async_remote_copy(
                src_ref=src,
                dst_ref=dst,
                send_sem=send_sems.at[stage, i],
                recv_sem=recv_sems.at[stage, i],
                device_id=target,
                device_id_type=MESH,
            )
            out.append((go, come, copy))
        return out

    def begin(plans):
        for go, _, copy in plans:
            pl.when(go)(copy.start)

    def receive(plans):
        for _, come, copy in plans:
            pl.when(come)(copy.wait_recv)

    def drain(plans):
        for go, _, copy in plans:
            pl.when(go)(copy.wait_send)

    pl.semaphore_wait(barrier, devices - 1)
    exchange = [faces(stage) for stage in range(3)]
    begin(exchange[0])
    for copy in loads[:first_loads]:
        copy.wait()

    lane = lax.broadcasted_iota(jnp.int32, (ny, LANES), 1)
    spans = [slice(h * LANES, (h + 1) * LANES) for h in range(halves)]

    def gathered(stage, x):
        acc = [[source[k, x, :, s] for s in spans] for k in range(nvar)]
        centres = []
        for e in range(nvar):
            centre = [fields[stage, e, x + 1, h, PAD : PAD + ny, :] for h in range(halves)]
            centres.append(centre)
            up = [pltpu.roll(c, LANES - 1, 1) for c in centre] + [jnp.zeros((ny, LANES), jnp.float32)]
            down = [jnp.zeros((ny, LANES), jnp.float32)] + [pltpu.roll(c, 1, 1) for c in centre]
            shifted = (
                [fields[stage, e, x + 2, h, PAD : PAD + ny, :] for h in range(halves)],
                [fields[stage, e, x, h, PAD : PAD + ny, :] for h in range(halves)],
                [fields[stage, e, x + 1, h, PAD + 1 : PAD + ny + 1, :] for h in range(halves)],
                [fields[stage, e, x + 1, h, PAD - 1 : PAD + ny - 1, :] for h in range(halves)],
                [jnp.where(lane == LANES - 1, up[h + 1], up[h]) for h in range(halves)],
                [jnp.where(lane == 0, down[h], down[h + 1]) for h in range(halves)],
            )
            for d in range(6):
                for k in range(nvar):
                    scale = flux[0, d, e, k]
                    for h in range(halves):
                        acc[k][h] = acc[k][h] + scale * shifted[d][h]
        return acc, centres

    def relax(stage, x, carry):
        acc, centres = gathered(stage, x)
        step = [RELAX / diagonal[x, :, s] for s in spans]
        total = [None] * halves
        for k in range(nvar):
            for h in range(halves):
                value = (1.0 - RELAX) * centres[k][h] + step[h] * acc[k][h]
                fields[stage + 1, k, x + 1, h, PAD : PAD + ny, :] = value
                if stage == 1:
                    smoothed_out[0, k, x, :, spans[h]] = value
                    term = value * sensitivity[k, x, :, spans[h]].astype(jnp.float32)
                    total[h] = term if k == 0 else total[h] + term
        if stage == 1:
            for h in range(halves):
                surface[x, :, spans[h]] = total[h] * mask[x, :, spans[h]].astype(jnp.float32)
        return carry

    def settle(x, carry):
        acc, centres = gathered(2, x)
        for k in range(nvar):
            for h in range(halves):
                value = acc[k][h] - diagonal[x, :, spans[h]] * centres[k][h]
                residual_out[0, k, x, :, spans[h]] = value
        return carry

    receive(exchange[0])
    lax.fori_loop(0, nx, functools.partial(relax, 0), 0)
    begin(exchange[1])
    for copy in loads[first_loads:]:
        copy.wait()
    receive(exchange[1])
    lax.fori_loop(0, nx, functools.partial(relax, 1), 0)
    begin(exchange[2])

    def split(value):
        high = value.astype(jnp.bfloat16)
        return high, (value - high.astype(jnp.float32)).astype(jnp.bfloat16)

    dot = functools.partial(jnp.dot, preferred_element_type=jnp.float32)
    basis_high, basis_low = split(basis[...])
    surface_high, surface_low = split(surface[...].reshape(nx * ny, nz))
    projected = (
        dot(surface_high, basis_high) + dot(surface_high, basis_low) + dot(surface_low, basis_high)
    )
    lines = NDES // LANES
    line = lax.broadcasted_iota(jnp.int32, (lines, ny), 0)
    wanted = jnp.concatenate([2 * line, 2 * line + 1, 2 * line - 1], axis=0)
    looked = jnp.zeros((3 * lines, LANES), jnp.float32)
    for x in range(nx):
        onehot = (wanted == slots[x : x + 1, :]).astype(jnp.float32).astype(jnp.bfloat16)
        high, low = split(projected[x * ny : (x + 1) * ny])
        looked = looked + dot(onehot, high) + dot(onehot, low)
    turned = pltpu.roll(looked[lines:], LANES // 2, 1)
    column = lax.broadcasted_iota(jnp.int32, (lines, LANES), 1)
    gradient = looked[:lines] + jnp.where(column < LANES // 2, turned[lines:], turned[:lines])
    weight_sum = weights[0]
    for c in range(1, n_cond):
        weight_sum = weight_sum + weights[c]
    share = jnp.full((1, LANES), weights[ci], jnp.int32).astype(jnp.float32) / jnp.full(
        (1, LANES), weight_sum, jnp.int32
    ).astype(jnp.float32)
    gradient = gradient * share
    for g in range(lines // rows):
        pieces[g] = gradient[g * rows : (g + 1) * rows]

    def group(gx, yz):
        return (gx * n_yz + yz) * per_owner // (rows * LANES)

    def give(step, carry):
        c, gx, yz = place((me + step) % devices)
        pltpu.make_async_remote_copy(
            src_ref=pieces.at[group(gx, yz)],
            dst_ref=arrived.at[me],
            send_sem=piece_sems.at[0],
            recv_sem=piece_sems.at[1],
            device_id=(c, gx, yz),
            device_id_type=MESH,
        ).start()
        return carry

    arrived[me] = pieces[group(xi, yi)]
    lax.fori_loop(1, devices, give, 0)

    receive(exchange[2])
    lax.fori_loop(0, nx, settle, 0)

    others = arrived.at[pl.ds(0, devices - 1)]
    for i in range(2):
        pltpu.make_async_copy(others, others, piece_sems.at[i]).wait()
    gradient_out[...] = jnp.sum(arrived[...], axis=0)
    for plans in exchange:
        drain(plans)


def local(
    adjoint,
    objective_gradient,
    diagonal,
    flux_blocks,
    flux_sensitivity,
    surface_mask,
    patch_band_slot,
    design_basis,
    condition_weights,
):
    sizes = tuple(lax.axis_size(axis) for axis in ("cond", "gx", "yz"))
    devices = sizes[0] * sizes[1] * sizes[2]
    _, nvar, nx, ny, nz = adjoint.shape
    halves = nz // LANES
    per_owner = NDES // (sizes[1] * sizes[2])
    rows = max(1, per_owner // LANES)
    f32 = jnp.float32
    hbm = pl.BlockSpec(memory_space=pltpu.MemorySpace.HBM)
    smem = pl.BlockSpec(memory_space=pltpu.MemorySpace.SMEM)
    vmem = pl.BlockSpec(memory_space=pltpu.MemorySpace.VMEM)
    faces = 4 * halves
    smoothed, residual, gradient = pl.pallas_call(
        functools.partial(kernel, sizes),
        out_shape=(
            jax.ShapeDtypeStruct(adjoint.shape, f32),
            jax.ShapeDtypeStruct(adjoint.shape, f32),
            jax.ShapeDtypeStruct((rows, LANES), f32),
        ),
        in_specs=[hbm, hbm, hbm, smem, hbm, hbm, hbm, hbm, smem],
        out_specs=(vmem, vmem, vmem),
        scratch_shapes=[
            pltpu.VMEM((3, nvar, nx + 2, halves, ny + 2 * PAD, LANES), f32),
            pltpu.VMEM((nvar, nx, ny, nz), f32),
            pltpu.VMEM((nx, ny, nz), f32),
            pltpu.VMEM((nvar, nx, ny, nz), jnp.bfloat16),
            pltpu.VMEM((nx, ny, nz), jnp.int32),
            pltpu.VMEM((nx, ny), jnp.int32),
            pltpu.VMEM(design_basis.shape, f32),
            pltpu.VMEM((nx, ny, nz), f32),
            pltpu.VMEM((NDES // (rows * LANES), rows, LANES), f32),
            pltpu.VMEM((devices, rows, LANES), f32),
            pltpu.SemaphoreType.DMA((6 + halves,)),
            pltpu.SemaphoreType.DMA((3, faces)),
            pltpu.SemaphoreType.DMA((3, faces)),
            pltpu.SemaphoreType.DMA((2,)),
        ],
        compiler_params=pltpu.CompilerParams(
            collective_id=0, has_side_effects=True
        ),
    )(
        adjoint,
        objective_gradient,
        diagonal,
        flux_blocks,
        flux_sensitivity,
        surface_mask,
        patch_band_slot,
        design_basis,
        condition_weights,
    )
    flat = gradient.reshape(-1)
    if per_owner < flat.shape[0]:
        owner = lax.axis_index(("gx", "yz"))
        flat = lax.dynamic_slice_in_dim(flat, (owner * per_owner) % flat.shape[0], per_owner, 0)
    return smoothed, residual, flat


def solution(mesh):
    placed = (
        P("cond", None, "gx", "yz", None),
        P("cond", None, "gx", "yz", None),
        P("gx", "yz", None),
        P("cond", None, None, None),
        P("cond", None, "gx", "yz", None),
        P("gx", "yz", None),
        P("gx", "yz"),
        P(),
        P(),
    )
    return jax.shard_map(
        local,
        mesh=mesh,
        in_specs=placed,
        out_specs=(
            P("cond", None, "gx", "yz", None),
            P("cond", None, "gx", "yz", None),
            P(("gx", "yz")),
        ),
        check_vma=False,
    )
```

```python
import functools

import jax
import jax.numpy as jnp
from jax import lax
from jax.experimental import pallas as pl
from jax.experimental.pallas import tpu as pltpu
from jax.sharding import PartitionSpec as P

NDES = 4096
RELAX = 0.8
LANES = 128
PAD = 8
MESH = pl.DeviceIdType.MESH


def kernel(
    sizes,
    adjoint,
    source_hbm,
    diagonal_hbm,
    flux,
    sensitivity_hbm,
    mask_hbm,
    slots_hbm,
    basis_hbm,
    weights,
    smoothed_out,
    residual_out,
    gradient_out,
    fields,
    source,
    diagonal,
    sensitivity,
    mask,
    slots,
    basis,
    surface,
    pieces,
    arrived,
    local_sems,
    plane_sems,
    first_sems,
    row_sems,
    face_sems,
    piece_sems,
):
    n_cond, n_gx, n_yz = sizes
    devices = n_cond * n_gx * n_yz
    nvar, nx, ny, nz = source.shape
    halves = nz // LANES
    rows = pieces.shape[1]
    per_owner = NDES // (n_gx * n_yz)
    ci, xi, yi = lax.axis_index("cond"), lax.axis_index("gx"), lax.axis_index("yz")
    me = (ci * n_gx + xi) * n_yz + yi

    def place(flat):
        return (flat // (n_gx * n_yz), (flat // n_yz) % n_gx, flat % n_yz)

    barrier = pltpu.get_barrier_semaphore()

    def for_others(action):
        if devices <= 64:
            here = (ci, xi, yi)
            turns = [[(p + t) % n for t in range(n)] for p, n in zip(here, sizes)]
            for dy in range(n_yz):
                for dx in range(n_gx):
                    for dc in range(n_cond):
                        if dc or dx or dy:
                            action(turns[0][dc], turns[1][dx], turns[2][dy])
        else:

            def step(t, carry):
                action(*place((me + t) % devices))
                return carry

            lax.fori_loop(1, devices, step, 0)

    def greet(c, gx, yz):
        pl.semaphore_signal(barrier, inc=1, device_id=(c, gx, yz), device_id_type=MESH)

    for_others(greet)
    inner_y = pl.ds(PAD, ny)

    def plane_loads(x):
        pairs = [
            (
                adjoint.at[0, :, x, :, pl.ds(h * LANES, LANES)],
                fields.at[0, :, x + 1, h, inner_y, :],
            )
            for h in range(halves)
        ]
        pairs.append((source_hbm.at[0, :, x], source.at[:, x]))
        pairs.append((diagonal_hbm.at[x], diagonal.at[x]))
        return [
            pltpu.make_async_copy(src, dst, plane_sems.at[i, x])
            for i, (src, dst) in enumerate(pairs)
        ]

    late_loads = [
        pltpu.make_async_copy(src, dst, local_sems.at[i])
        for i, (src, dst) in enumerate(
            (
                (sensitivity_hbm.at[0], sensitivity),
                (mask_hbm, mask),
                (slots_hbm, slots),
                (basis_hbm, basis),
            )
        )
    ]
    for x in range(nx):
        for copy in plane_loads(x):
            copy.start()
    for copy in late_loads:
        copy.start()

    has_before_x, has_after_x = xi > 0, xi < n_gx - 1
    has_before_y, has_after_y = yi > 0, yi < n_yz - 1

    blank_x = jnp.zeros((nvar, halves, ny, LANES), jnp.float32)
    blank_y = jnp.zeros((nvar, nx, halves, 1, LANES), jnp.float32)

    def clear_x(stage, x):
        fields[stage, :, x, :, PAD : PAD + ny, :] = blank_x

    def clear_y(stage, y):
        fields[stage, :, 1 : nx + 1, :, y : y + 1, :] = blank_y

    for stage in range(3):
        pl.when(xi == 0)(functools.partial(clear_x, stage, 0))
        pl.when(xi == n_gx - 1)(functools.partial(clear_x, stage, nx + 1))
        pl.when(yi == 0)(functools.partial(clear_y, stage, PAD - 1))
        pl.when(yi == n_yz - 1)(functools.partial(clear_y, stage, PAD + ny))

    def remote(src, dst, sems, target):
        return pltpu.make_async_remote_copy(
            src_ref=src,
            dst_ref=dst,
            send_sem=sems[0],
            recv_sem=sems[1],
            device_id=target,
            device_id_type=MESH,
        )

    after_x, before_x = (ci, xi + 1, yi), (ci, xi - 1, yi)
    after_y, before_y = (ci, xi, yi + 1), (ci, xi, yi - 1)

    first_y, first_x = [], []
    for h in range(halves):
        lanes = pl.ds(h * LANES, LANES)

        def sems(way, h=h):
            return first_sems.at[0, way, h], first_sems.at[1, way, h]

        inner_x = pl.ds(1, nx)
        first_y.append((has_after_y, has_before_y, remote(
            adjoint.at[0, :, :, pl.ds(ny - 1, 1), lanes],
            fields.at[0, :, inner_x, h, pl.ds(PAD - 1, 1), :], sems(0), after_y)))
        first_y.append((has_before_y, has_after_y, remote(
            adjoint.at[0, :, :, pl.ds(0, 1), lanes],
            fields.at[0, :, inner_x, h, pl.ds(PAD + ny, 1), :], sems(1), before_y)))
        first_x.append((has_after_x, has_before_x, remote(
            adjoint.at[0, :, nx - 1, :, lanes],
            fields.at[0, :, 0, h, inner_y, :], sems(2), after_x)))
        first_x.append((has_before_x, has_after_x, remote(
            adjoint.at[0, :, 0, :, lanes],
            fields.at[0, :, nx + 1, h, inner_y, :], sems(3), before_x)))

    def row_copies(stage, x):
        def sems(way):
            return row_sems.at[stage - 1, 0, way, x], row_sems.at[stage - 1, 1, way, x]

        def row(y):
            return fields.at[stage, :, x + 1, :, pl.ds(y, 1), :]

        return [
            (has_after_y, has_before_y, remote(row(PAD + ny - 1), row(PAD - 1), sems(0), after_y)),
            (has_before_y, has_after_y, remote(row(PAD), row(PAD + ny), sems(1), before_y)),
        ]

    def face_copies(stage):
        def sems(way):
            return face_sems.at[stage - 1, 0, way], face_sems.at[stage - 1, 1, way]

        def face(x):
            return fields.at[stage, :, x, :, inner_y, :]

        return [
            (has_after_x, has_before_x, remote(face(nx), face(0), sems(0), after_x)),
            (has_before_x, has_after_x, remote(face(1), face(nx + 1), sems(1), before_x)),
        ]

    def begin(plans):
        for go, _, copy in plans:
            pl.when(go)(copy.start)

    def receive(plans):
        for _, come, copy in plans:
            pl.when(come)(copy.wait_recv)

    def drain(plans):
        for go, _, copy in plans:
            pl.when(go)(copy.wait_send)

    pl.semaphore_wait(barrier, devices - 1)
    begin(first_y)
    begin(first_x)

    def plane_of(step):
        return jnp.where(step < nx - 2, step + 1, jnp.where(step == nx - 2, 0, nx - 1))

    lane = lax.broadcasted_iota(jnp.int32, (ny, LANES), 1)
    spans = [slice(h * LANES, (h + 1) * LANES) for h in range(halves)]

    def gathered(stage, x):
        acc = [[source[k, x, :, s] for s in spans] for k in range(nvar)]
        centres = []
        for e in range(nvar):
            centre = [fields[stage, e, x + 1, h, PAD : PAD + ny, :] for h in range(halves)]
            centres.append(centre)
            up = [pltpu.roll(c, LANES - 1, 1) for c in centre] + [jnp.zeros((ny, LANES), jnp.float32)]
            down = [jnp.zeros((ny, LANES), jnp.float32)] + [pltpu.roll(c, 1, 1) for c in centre]
            shifted = (
                [fields[stage, e, x + 2, h, PAD : PAD + ny, :] for h in range(halves)],
                [fields[stage, e, x, h, PAD : PAD + ny, :] for h in range(halves)],
                [fields[stage, e, x + 1, h, PAD + 1 : PAD + ny + 1, :] for h in range(halves)],
                [fields[stage, e, x + 1, h, PAD - 1 : PAD + ny - 1, :] for h in range(halves)],
                [jnp.where(lane == LANES - 1, up[h + 1], up[h]) for h in range(halves)],
                [jnp.where(lane == 0, down[h], down[h + 1]) for h in range(halves)],
            )
            for d in range(6):
                for k in range(nvar):
                    scale = flux[e, k, 0, d]
                    for h in range(halves):
                        acc[k][h] = acc[k][h] + scale * shifted[d][h]
        return acc, centres

    def ready(stage, step):
        x = plane_of(step)
        if stage == 0:

            @pl.when(step < nx - 2)
            def _():
                for copy in plane_loads(step + 2):
                    copy.wait()

        else:
            receive(row_copies(stage, x))

        @pl.when(step == nx - 2)
        def _():
            receive(first_x if stage == 0 else face_copies(stage))

        return x

    def relax(stage, step_index, carry):
        x = ready(stage, step_index)
        acc, centres = gathered(stage, x)
        step = [RELAX / diagonal[x, :, s] for s in spans]
        total = [None] * halves
        for k in range(nvar):
            for h in range(halves):
                value = (1.0 - RELAX) * centres[k][h] + step[h] * acc[k][h]
                fields[stage + 1, k, x + 1, h, PAD : PAD + ny, :] = value
                if stage == 1:
                    smoothed_out[0, k, x, :, spans[h]] = value
                    term = value * sensitivity[k, x, :, spans[h]].astype(jnp.float32)
                    total[h] = term if k == 0 else total[h] + term
        if stage == 1:
            for h in range(halves):
                surface[x, :, spans[h]] = total[h] * mask[x, :, spans[h]].astype(jnp.float32)
        begin(row_copies(stage + 1, x))
        up_face, down_face = face_copies(stage + 1)
        pl.when(x == nx - 1)(functools.partial(begin, [up_face]))
        pl.when(x == 0)(functools.partial(begin, [down_face]))
        return carry

    def settle(step_index, carry):
        x = ready(2, step_index)
        acc, centres = gathered(2, x)
        for k in range(nvar):
            for h in range(halves):
                value = acc[k][h] - diagonal[x, :, spans[h]] * centres[k][h]
                residual_out[0, k, x, :, spans[h]] = value
        return carry

    for x in range(2):
        for copy in plane_loads(x):
            copy.wait()
    receive(first_y)
    lax.fori_loop(0, nx, functools.partial(relax, 0), 0)
    for copy in late_loads:
        copy.wait()
    lax.fori_loop(0, nx, functools.partial(relax, 1), 0)

    def split(value):
        high = value.astype(jnp.bfloat16)
        return high, (value - high.astype(jnp.float32)).astype(jnp.bfloat16)

    dot = functools.partial(jnp.dot, preferred_element_type=jnp.float32)
    basis_high, basis_low = split(basis[...])
    surface_high, surface_low = split(surface[...].reshape(nx * ny, nz))
    projected = (
        dot(surface_high, basis_high) + dot(surface_high, basis_low) + dot(surface_low, basis_high)
    )
    lines = NDES // LANES
    line = lax.broadcasted_iota(jnp.int32, (lines, ny), 0)
    wanted = jnp.concatenate([2 * line, 2 * line + 1, 2 * line - 1], axis=0)
    looked = jnp.zeros((3 * lines, LANES), jnp.float32)
    for x in range(nx):
        onehot = (wanted == slots[x : x + 1, :]).astype(jnp.float32).astype(jnp.bfloat16)
        high, low = split(projected[x * ny : (x + 1) * ny])
        looked = looked + dot(onehot, high) + dot(onehot, low)
    turned = pltpu.roll(looked[lines:], LANES // 2, 1)
    column = lax.broadcasted_iota(jnp.int32, (lines, LANES), 1)
    gradient = looked[:lines] + jnp.where(column < LANES // 2, turned[lines:], turned[:lines])
    weight_sum = weights[0]
    for c in range(1, n_cond):
        weight_sum = weight_sum + weights[c]
    share = jnp.full((1, LANES), weights[ci], jnp.int32).astype(jnp.float32) / jnp.full(
        (1, LANES), weight_sum, jnp.int32
    ).astype(jnp.float32)
    gradient = gradient * share
    for g in range(lines // rows):
        pieces[g] = gradient[g * rows : (g + 1) * rows]

    def group(gx, yz):
        return (gx * n_yz + yz) * per_owner // (rows * LANES)

    def give(c, gx, yz):
        remote(
            pieces.at[group(gx, yz)],
            arrived.at[me],
            (piece_sems.at[0], piece_sems.at[1]),
            (c, gx, yz),
        ).start()

    arrived[me] = pieces[group(xi, yi)]
    for_others(give)
    lax.fori_loop(0, nx, settle, 0)

    others = arrived.at[pl.ds(0, devices - 1)]
    for i in range(2):
        pltpu.make_async_copy(others, others, piece_sems.at[i]).wait()
    gradient_out[...] = jnp.sum(arrived[...], axis=0)
    drain(first_y)
    drain(first_x)
    for stage in (1, 2):
        drain(face_copies(stage))

        def drain_row(x, carry, stage=stage):
            drain(row_copies(stage, x))
            return carry

        lax.fori_loop(0, nx, drain_row, 0)


def local(
    adjoint,
    objective_gradient,
    diagonal,
    flux_blocks,
    flux_sensitivity,
    surface_mask,
    patch_band_slot,
    design_basis,
    condition_weights,
):
    sizes = tuple(lax.axis_size(axis) for axis in ("cond", "gx", "yz"))
    devices = sizes[0] * sizes[1] * sizes[2]
    _, nvar, nx, ny, nz = adjoint.shape
    halves = nz // LANES
    per_owner = NDES // (sizes[1] * sizes[2])
    rows = max(1, per_owner // LANES)
    f32 = jnp.float32
    hbm = pl.BlockSpec(memory_space=pltpu.MemorySpace.HBM)
    smem = pl.BlockSpec(memory_space=pltpu.MemorySpace.SMEM)
    vmem = pl.BlockSpec(memory_space=pltpu.MemorySpace.VMEM)
    smoothed, residual, gradient = pl.pallas_call(
        functools.partial(kernel, sizes),
        out_shape=(
            pltpu.VMEM(adjoint.shape, f32),
            pltpu.VMEM(adjoint.shape, f32),
            pltpu.VMEM((rows, LANES), f32),
        ),
        in_specs=[hbm, hbm, hbm, smem, hbm, hbm, hbm, hbm, smem],
        out_specs=(vmem, vmem, vmem),
        scratch_shapes=[
            pltpu.VMEM((3, nvar, nx + 2, halves, ny + 2 * PAD, LANES), f32),
            pltpu.VMEM((nvar, nx, ny, nz), f32),
            pltpu.VMEM((nx, ny, nz), f32),
            pltpu.VMEM((nvar, nx, ny, nz), jnp.bfloat16),
            pltpu.VMEM((nx, ny, nz), jnp.int32),
            pltpu.VMEM((nx, ny), jnp.int32),
            pltpu.VMEM(design_basis.shape, f32),
            pltpu.VMEM((nx, ny, nz), f32),
            pltpu.VMEM((NDES // (rows * LANES), rows, LANES), f32),
            pltpu.VMEM((devices, rows, LANES), f32),
            pltpu.SemaphoreType.DMA((4,)),
            pltpu.SemaphoreType.DMA((2 + halves, nx)),
            pltpu.SemaphoreType.DMA((2, 4, halves)),
            pltpu.SemaphoreType.DMA((2, 2, 2, nx)),
            pltpu.SemaphoreType.DMA((2, 2, 2)),
            pltpu.SemaphoreType.DMA((2,)),
        ],
        compiler_params=pltpu.CompilerParams(
            collective_id=0, has_side_effects=True, vmem_limit_bytes=67043328 - 2 * adjoint.size * 4 - 2**16
        ),
    )(
        adjoint,
        objective_gradient,
        diagonal,
        jnp.transpose(flux_blocks, (2, 3, 0, 1)),
        flux_sensitivity,
        surface_mask,
        patch_band_slot,
        design_basis,
        condition_weights,
    )
    flat = gradient.reshape(-1)
    if per_owner < flat.shape[0]:
        owner = lax.axis_index(("gx", "yz"))
        flat = lax.dynamic_slice_in_dim(flat, (owner * per_owner) % flat.shape[0], per_owner, 0)
    return smoothed, residual, flat


def solution(mesh):
    placed = (
        P("cond", None, "gx", "yz", None),
        P("cond", None, "gx", "yz", None),
        P("gx", "yz", None),
        P("cond", None, None, None),
        P("cond", None, "gx", "yz", None),
        P("gx", "yz", None),
        P("gx", "yz"),
        P(),
        P(),
    )
    return jax.shard_map(
        local,
        mesh=mesh,
        in_specs=placed,
        out_specs=(
            P("cond", None, "gx", "yz", None),
            P("cond", None, "gx", "yz", None),
            P(("gx", "yz")),
        ),
        check_vma=False,
    )
```
